32 devices in a mesh: group: 2 (over core), fsdp: 4 (over z), tp: 4 (over y, x).
Axes of the slice: x: 2, y: 2, z: 4, core: 2. Of those that a mesh axis runs over, the one named last changes fastest.
Arguments:
- text_embeds: bfloat16 [4096, 8192], P(('group', 'fsdp'), 'tp'), may hold values from -6 to 6
- image_embeds: bfloat16 [2048, 8192], P(('group', 'fsdp'), 'tp'), may hold values from -6 to 6
- key_weight: bfloat16 [8192, 512], P(('group', 'fsdp')), may hold values from -0.0625 to 0.0625
- key_bias: float32 [512], P('tp'), may hold values from -3 to 3
- key_cot: bfloat16 [4096, 512], P(('group', 'fsdp')), may hold values from -6 to 6
- image_owner: int32 [2048], P(('group', 'fsdp')), may hold values from 0 to 7, as said below
- image_slot: int32 [4096], P(('group', 'fsdp')), may hold values from -1 to 511, as said below
- seq_lengths: int32 [16], P(('group', 'fsdp')), may hold values from 248 to 256, as said below
Outputs:
- key_rows: bfloat16 [4096, 512], P(('group', 'fsdp'), 'tp')
- text_grad: bfloat16 [4096, 8192], P(('group', 'fsdp'), 'tp')
- image_grad: bfloat16 [2048, 8192], P(('group', 'fsdp'), 'tp')
- weight_grad: float32 [8192, 512], P(('group', 'fsdp'), 'tp')
The draws below stay inside these ranges and needn't reach their ends.
Inputs may be any that keep to these rules, and one draw needn't show every extreme that they name: `image_owner`: A source block of 256 image tokens sends at most 64 of them to one owner, and some block sends exactly 64 to some owner; an owner takes at most 448 image tokens in all, and some owner takes exactly that many. Every image token has exactly one position, as step one says. `image_slot`: slots are distinct within an owner block, and image tokens sit only at live positions. `seq_lengths`: some sequence has length 256.
All inputs are finite; a program needn't handle non-finite values.
Results may differ from the reference program's by a relative error of at most 0.0046.
Values may be sent and summed in bfloat16 or wider, within the bound.
A program may use at most 64 MiB of HBM per device.

```python
import jax
import jax.numpy as jnp
from jax import lax

D = 8192
HEAD_DIM = 128
LENGTH = 256
SEQ_DEV = 2
KW = 512
UNITS = 8
LANG_DEV = 512
IMG_DEV = 256
CAP = 64
LANG_TOKENS = 4096
IMG_TOKENS = 2048


def layout_tables(key):
    base_key = jax.random.fold_in(key, 9137)
    subkeys = jax.random.split(base_key, 8)
    unit_count = UNITS
    quantum = LANG_DEV // (8 * UNITS)
    ordinal = jnp.arange(unit_count, dtype=jnp.int32)
    heavy_count = jax.random.randint(subkeys[0], (), 1, unit_count // 2 + 1)
    light_count = jax.random.randint(subkeys[1], (), 1, unit_count // 2 + 1)
    owner_sorted = jnp.where(ordinal < heavy_count, 6 * quantum, jnp.where(ordinal < unit_count - heavy_count, 3 * quantum, 0)).astype(jnp.int32)
    offset_sorted = jnp.where(ordinal < light_count, 2 * quantum, jnp.where(ordinal < unit_count - light_count, quantum, 0)).astype(jnp.int32)
    owner_load = owner_sorted[jax.random.permutation(subkeys[2], unit_count)]
    offset_load = offset_sorted[jax.random.permutation(subkeys[3], unit_count)]
    shift_index = (ordinal[None, :] - ordinal[:, None]) % unit_count
    counts = (owner_load[None, :] + offset_load[shift_index]).astype(jnp.int32)
    cum_owner = jnp.cumsum(counts, axis=1)
    token_index = jnp.arange(IMG_DEV, dtype=jnp.int32)
    owner_list = jnp.sum((cum_owner[:, None, :] <= token_index[None, :, None]).astype(jnp.int32), axis=2)
    row_keys = jax.random.split(subkeys[4], unit_count)
    row_perms = jax.vmap(lambda one_key: jax.random.permutation(one_key, IMG_DEV))(row_keys)
    owners = jnp.take_along_axis(owner_list, row_perms, axis=1).astype(jnp.int32)
    seq_total = unit_count * SEQ_DEV
    padding = jax.random.randint(subkeys[5], (seq_total,), 0, LENGTH // 32 + 1)
    full_one = jax.random.randint(subkeys[6], (), 0, seq_total)
    lengths = (LENGTH - jnp.where(jnp.arange(seq_total) == full_one, 0, padding)).astype(jnp.int32)
    within = jnp.arange(LANG_DEV, dtype=jnp.int32)
    live_table = within[None, :] % LENGTH < lengths.reshape(unit_count, SEQ_DEV)[:, within // LENGTH]
    place_keys = jax.random.split(subkeys[7], unit_count)
    place_perms = jax.vmap(lambda one_key: jax.random.permutation(one_key, LANG_DEV))(place_keys)
    live_perm = jnp.take_along_axis(live_table, place_perms, axis=1)
    arrival = jnp.cumsum(live_perm.astype(jnp.int32), axis=1) - 1
    incoming = jnp.sum(counts, axis=0)
    chosen = live_perm & (arrival < incoming[:, None])
    cum_source = jnp.cumsum(counts, axis=0).T
    source_ids = jnp.sum((cum_source[:, None, :] <= arrival[:, :, None]).astype(jnp.int32), axis=2)
    source_ids = jnp.clip(source_ids, 0, unit_count - 1)
    start_table = (jnp.cumsum(counts, axis=0) - counts).T
    source_start = jnp.take_along_axis(start_table, source_ids, axis=1)
    slot_value = jnp.where(chosen, source_ids * CAP + arrival - source_start, -1).astype(jnp.int32)
    slots = jnp.zeros((unit_count, LANG_DEV), jnp.int32).at[ordinal[:, None], place_perms].set(slot_value)
    return (owners.reshape(-1), slots.reshape(-1), lengths)


def draw_image_owner(key, part):
    return layout_tables(key)[0]


def draw_image_slot(key, part):
    return layout_tables(key)[1]


def draw_seq_lengths(key, part):
    return layout_tables(key)[2]


def spiked(values, rng, source, target, shards_of, factor):
    def block_of(dim):
        return (jnp.arange(values.shape[dim]) // (values.shape[dim] // shards_of)).reshape((-1,) + (1,) * (values.ndim - 1 - dim))

    near = jax.random.permutation(rng, shards_of)[block_of(target)]
    second = (block_of(target) + shards_of // 2) % shards_of
    return jnp.where((block_of(source) == near) | (block_of(source) == second), factor * values, values)


def levels(rng, dims, cuts, least, high):
    def one(axis_at, blocks):
        steps = jax.random.uniform(jax.random.fold_in(jax.random.fold_in(rng, 6), axis_at), (blocks,), jnp.float32, least / len(cuts), high / len(cuts))
        return jnp.repeat(jnp.exp(steps), dims[axis_at] // blocks).reshape((-1,) + (1,) * (len(dims) - axis_at - 1))

    factor_of = one(*cuts[0])
    for cut in cuts[1:]:
        factor_of = factor_of * one(*cut)
    return factor_of


def bell_draw(stream_key, shape, width, limit, cuts=(), kind=jnp.bfloat16):
    loudness = levels(stream_key, shape, cuts, -0.22, 0.18) if cuts else 1.0
    drawn = jax.random.normal(stream_key, shape, jnp.float32) * width * loudness
    return jnp.minimum(jnp.maximum(drawn, -limit), limit).astype(kind)


def heavy_noise(own_key, extent, width, reach, shards, heavy, held_as=jnp.bfloat16):
    result = width * jax.random.normal(own_key, extent, jnp.float32)
    if shards:
        result = result * levels(own_key, extent, shards, -0.22, 0.18)
    return jnp.clip(spiked(result, jax.random.fold_in(own_key, 3), *heavy), -reach, reach).astype(held_as)


def setup_inputs(seed: int = 0) -> dict:
    key_list = jax.random.split(jax.random.key(seed), 9)
    return {
        "text_embeds": heavy_noise(key_list[0], (LANG_TOKENS, D), 1.0, 6.0, ((0, 8), (1, 4)), (0, 1, 8, 2.0)),
        "image_embeds": bell_draw(key_list[1], (IMG_TOKENS, D), 1.0, 6.0, ((0, 8), (1, 4))),
        "key_weight": bell_draw(key_list[2], (D, KW), D ** -0.5, 0.0625, ((0, 8),)),
        "key_bias": bell_draw(key_list[3], (KW,), 0.5, 3.0, ((0, 4),), jnp.float32),
        "key_cot": bell_draw(key_list[4], (LANG_TOKENS, KW), 1.0, 6.0, ((0, 8),)),
        "image_owner": draw_image_owner(jax.random.fold_in(key_list[8], 71), 0),
        "image_slot": draw_image_slot(jax.random.fold_in(key_list[8], 71), 0),
        "seq_lengths": draw_seq_lengths(jax.random.fold_in(key_list[8], 71), 0),
    }


ROPE_BASE = 1000000.0


def angles(row_total):
    position = (jnp.arange(row_total, dtype=jnp.int32) % LENGTH).astype(jnp.float32)
    frequency = ROPE_BASE ** (-(jnp.arange(HEAD_DIM // 2, dtype=jnp.float32) * 2.0) / HEAD_DIM)
    angle_table = position[:, None] * frequency[None, :]
    return jnp.cos(angle_table), jnp.sin(angle_table)


def rotate(values, cosine, sine, direction):
    row_total = values.shape[0]
    by_head = values.reshape(row_total, -1, HEAD_DIM)
    half_dim = HEAD_DIM // 2
    front_half = by_head[..., :half_dim]
    second = by_head[..., half_dim:]
    cos_part = cosine[:, None, :]
    sin_part = direction * sine[:, None, :]
    rotated = jnp.concatenate([front_half * cos_part - second * sin_part, second * cos_part + front_half * sin_part], axis=-1)
    return rotated.reshape(row_total, -1)


def reference(text_embeds, image_embeds, key_weight, key_bias, key_cot, image_owner, image_slot, seq_lengths):
    unit_count = UNITS
    owners = image_owner.reshape(unit_count, IMG_DEV)
    ordinal = jnp.arange(unit_count, dtype=jnp.int32)
    marks = (owners[:, :, None] == ordinal[None, None, :]).astype(jnp.int32)
    before = jnp.cumsum(marks, axis=1) - marks
    owner_rank = jnp.sum(before * marks, axis=2)
    destination = owners * (unit_count * CAP) + ordinal[:, None] * CAP + owner_rank
    source_table = jnp.zeros((unit_count * unit_count * CAP,), jnp.int32).at[destination.reshape(-1)].set(jnp.arange(unit_count * IMG_DEV, dtype=jnp.int32))
    slots = image_slot.reshape(unit_count, LANG_DEV)
    is_image = (slots >= 0).reshape(-1)
    lookup = (ordinal[:, None] * (unit_count * CAP) + jnp.maximum(slots, 0)).reshape(-1)
    image_row = source_table[lookup]
    hidden = jnp.where(is_image[:, None], image_embeds[image_row], text_embeds)
    position = jnp.arange(LANG_TOKENS, dtype=jnp.int32)
    live_mask = ((position % LENGTH) < seq_lengths[position // LENGTH]).astype(jnp.float32)
    cosine, sine = angles(LANG_TOKENS)
    projected = jnp.dot(hidden, key_weight, preferred_element_type=jnp.float32) + key_bias
    key_rows = (rotate(projected, cosine, sine, 1.0) * live_mask[:, None]).astype(jnp.bfloat16)
    masked = key_cot.astype(jnp.float32) * live_mask[:, None]
    rotated_back = rotate(masked, cosine, sine, -1.0).astype(jnp.bfloat16)
    hidden_grad = lax.dot_general(rotated_back, key_weight, (((1,), (1,)), ((), ())), preferred_element_type=jnp.float32).astype(jnp.bfloat16)
    text_grad = jnp.where(is_image[:, None], jnp.zeros_like(hidden_grad), hidden_grad)
    token_place = jnp.zeros((unit_count * IMG_DEV,), jnp.int32).at[jnp.where(is_image, image_row, unit_count * IMG_DEV)].set(position, mode="drop")
    image_grad = hidden_grad[token_place]
    weight_grad = lax.dot_general(hidden, rotated_back, (((0,), (0,)), ((), ())), preferred_element_type=jnp.float32) / LANG_DEV
    return key_rows, text_grad, image_grad, weight_grad
```

```python
import jax
import jax.numpy as jnp
from jax import lax
from jax.sharding import PartitionSpec as P

HEAD_DIM = 128
LENGTH = 256


ROPE_BASE = 1000000.0


def angles(row_total):
    position = (jnp.arange(row_total, dtype=jnp.int32) % LENGTH).astype(jnp.float32)
    frequency = ROPE_BASE ** (-(jnp.arange(HEAD_DIM // 2, dtype=jnp.float32) * 2.0) / HEAD_DIM)
    angle_table = position[:, None] * frequency[None, :]
    return (jnp.cos(angle_table), jnp.sin(angle_table))


def rotate(values, cosine, sine, direction):
    row_total = values.shape[0]
    by_head = values.reshape(row_total, -1, HEAD_DIM)
    half_dim = HEAD_DIM // 2
    front_half = by_head[..., :half_dim]
    second = by_head[..., half_dim:]
    cos_part = cosine[:, None, :]
    sin_part = direction * sine[:, None, :]
    rotated = jnp.concatenate(
        [front_half * cos_part - second * sin_part, second * cos_part + front_half * sin_part],
        axis=-1,
    )
    return rotated.reshape(row_total, -1)


def send_slots(owners, unit_count, capacity):
    onehot_marks = (owners[:, None] == jnp.arange(unit_count, dtype=jnp.int32)[None, :]).astype(
        jnp.int32
    )
    before = jnp.cumsum(onehot_marks, axis=0) - onehot_marks
    owner_rank = jnp.sum(before * onehot_marks, axis=1)
    return owners * capacity + owner_rank


def per_device(
    text_embeds, image_embeds, key_weight, key_bias, key_cot, image_owner, image_slot, seq_lengths
):
    row_count, columns = text_embeds.shape
    image_count = image_embeds.shape[0]
    units = ("group", "fsdp")
    core_count = lax.axis_size("group")
    fsdp_count = lax.axis_size("fsdp")
    tp_count = lax.axis_size("tp")
    unit_count = core_count * fsdp_count
    capacity = row_count // unit_count
    slot_count = unit_count * capacity
    head_cols = key_bias.shape[0]
    key_cols = head_cols * tp_count
    weight_block = key_weight.shape[0]
    halves = unit_count // tp_count
    tp_index = lax.axis_index("tp")

    position = jnp.arange(row_count, dtype=jnp.int32)
    seq_ids = position // LENGTH
    seq_marks = seq_ids[:, None] == jnp.arange(seq_lengths.shape[0], dtype=jnp.int32)[None, :]
    live_limit = jnp.sum(jnp.where(seq_marks, seq_lengths[None, :], 0), axis=1)
    live_mask = (position % LENGTH < live_limit).astype(jnp.float32)
    cosine, sine = angles(row_count)
    masked = key_cot.astype(jnp.float32) * live_mask[:, None]
    rotated_back = rotate(masked, cosine, sine, -1.0).astype(jnp.bfloat16)
    is_image = image_slot >= 0
    text_back = jnp.where(is_image[:, None], jnp.zeros_like(rotated_back), rotated_back)

    slot_ids = jnp.arange(slot_count, dtype=jnp.int32)
    place = (image_slot[:, None] == slot_ids[None, :]).astype(jnp.bfloat16)
    returning = lax.dot_general(
        place, rotated_back, (((0,), (0,)), ((), ())), preferred_element_type=jnp.float32
    ).astype(jnp.bfloat16)
    returned = lax.all_to_all(
        returning.reshape(unit_count, capacity, key_cols), units, split_axis=0, concat_axis=0,
        tiled=True,
    ).reshape(slot_count, key_cols)
    slots_out = send_slots(image_owner, unit_count, capacity)
    pick = (slots_out[:, None] == slot_ids[None, :]).astype(jnp.bfloat16)
    image_back = jnp.dot(pick, returned, preferred_element_type=jnp.float32).astype(jnp.bfloat16)

    piece_rows = weight_block // tp_count
    own_piece = lax.dynamic_slice_in_dim(key_weight, tp_index * piece_rows, piece_rows, 0)
    moves = []
    for unit in range(unit_count):
        for part in range(tp_count):
            target = (unit % halves) * tp_count + part
            moves.append((unit * tp_count + part, target * tp_count + unit // halves))
    own_piece = lax.ppermute(own_piece, units + ("tp",), moves)
    weight_rows = lax.all_gather(own_piece, units, axis=0, tiled=True)

    weight_part = lax.dot_general(
        text_embeds, text_back, (((0,), (0,)), ((), ())), preferred_element_type=jnp.float32
    )
    weight_part = (
        weight_part
        + lax.dot_general(
            image_embeds, image_back, (((0,), (0,)), ((), ())), preferred_element_type=jnp.float32
        )
    ).astype(jnp.bfloat16)
    weight_part = weight_part.reshape(halves, weight_block, tp_count, head_cols)
    weight_part = weight_part.transpose(0, 2, 1, 3).reshape(unit_count, weight_block, head_cols)
    shares = lax.all_to_all(weight_part, units, split_axis=0, concat_axis=0, tiled=True)
    weight_grad = jnp.sum(shares.astype(jnp.float32), axis=0) / row_count
    weight_grad = lax.ppermute(weight_grad, units + ("tp",), [(b, a) for a, b in moves])

    text_part = jnp.dot(text_embeds, weight_rows, preferred_element_type=jnp.float32)
    image_part = jnp.dot(image_embeds, weight_rows, preferred_element_type=jnp.float32)
    both = jnp.concatenate(
        [text_part.astype(jnp.bfloat16), image_part.astype(jnp.bfloat16)], axis=0
    )
    both = both.reshape(row_count + image_count, tp_count, head_cols).transpose(1, 0, 2)
    both = lax.all_to_all(both, "tp", split_axis=0, concat_axis=0, tiled=True)
    both = jnp.sum(both.astype(jnp.float32), axis=0)
    image_proj = both[row_count:].astype(jnp.bfloat16)
    outgoing = lax.dot_general(
        pick, image_proj, (((0,), (0,)), ((), ())), preferred_element_type=jnp.float32
    ).astype(jnp.bfloat16)
    received = lax.all_to_all(
        outgoing.reshape(unit_count, capacity, head_cols), units, split_axis=0, concat_axis=0,
        tiled=True,
    ).reshape(slot_count, head_cols)
    placed = jnp.dot(place, received, preferred_element_type=jnp.float32)
    projected = jnp.where(is_image[:, None], placed, both[:row_count]) + key_bias
    key_rows = (rotate(projected, cosine, sine, 1.0) * live_mask[:, None]).astype(jnp.bfloat16)

    contract = (((1,), (1,)), ((), ()))
    text_grad = lax.dot_general(
        text_back, weight_rows, contract, preferred_element_type=jnp.float32
    ).astype(jnp.bfloat16)
    image_grad = lax.dot_general(
        image_back, weight_rows, contract, preferred_element_type=jnp.float32
    ).astype(jnp.bfloat16)
    return (key_rows, text_grad, image_grad, weight_grad)


def solution(mesh):
    in_specs = (
        P(("group", "fsdp"), "tp"),
        P(("group", "fsdp"), "tp"),
        P(("group", "fsdp"), None),
        P("tp"),
        P(("group", "fsdp"), None),
        P(("group", "fsdp")),
        P(("group", "fsdp")),
        P(("group", "fsdp")),
    )
    out_specs = (
        P(("group", "fsdp"), "tp"),
        P(("group", "fsdp"), "tp"),
        P(("group", "fsdp"), "tp"),
        P(("group", "fsdp"), "tp"),
    )
    return jax.shard_map(
        per_device, mesh=mesh, in_specs=in_specs, out_specs=out_specs, check_vma=False
    )
```

```python
import jax
import jax.numpy as jnp
from jax import lax
from jax.experimental import pallas as pl
from jax.experimental.pallas import tpu as pltpu
from jax.sharding import PartitionSpec as P

HEAD_DIM = 128
LENGTH = 256


ROPE_BASE = 1000000.0


def angles(row_total):
    position = (jnp.arange(row_total, dtype=jnp.int32) % LENGTH).astype(jnp.float32)
    frequency = ROPE_BASE ** (-(jnp.arange(HEAD_DIM // 2, dtype=jnp.float32) * 2.0) / HEAD_DIM)
    angle_table = position[:, None] * frequency[None, :]
    return (jnp.cos(angle_table), jnp.sin(angle_table))


def rotate(values, cosine, sine, direction):
    row_total = values.shape[0]
    by_head = values.reshape(row_total, -1, HEAD_DIM)
    half_dim = HEAD_DIM // 2
    front_half = by_head[..., :half_dim]
    second = by_head[..., half_dim:]
    cos_part = cosine[:, None, :]
    sin_part = direction * sine[:, None, :]
    rotated = jnp.concatenate(
        [front_half * cos_part - second * sin_part, second * cos_part + front_half * sin_part],
        axis=-1,
    )
    return rotated.reshape(row_total, -1)


def send_slots(owners, unit_count, capacity):
    onehot_marks = (owners[:, None] == jnp.arange(unit_count, dtype=jnp.int32)[None, :]).astype(
        jnp.int32
    )
    before = jnp.cumsum(onehot_marks, axis=0) - onehot_marks
    owner_rank = jnp.sum(before * onehot_marks, axis=1)
    return owners * capacity + owner_rank


def share_kernel(text_ref, image_ref, back_ref, image_back_ref, out_ref):
    contract = (((0,), (0,)), ((), ()))
    part = lax.dot_general(
        text_ref[...], back_ref[...], contract, preferred_element_type=jnp.float32
    ) + lax.dot_general(
        image_ref[...], image_back_ref[...], contract, preferred_element_type=jnp.float32
    )
    part = part.astype(out_ref.dtype)
    width = out_ref.shape[2]
    for head in range(out_ref.shape[0]):
        out_ref[head] = part[:, head * width : (head + 1) * width]


def weight_shares(text, image, back, image_back, head_cols):
    columns = text.shape[1]
    heads = back.shape[1] // head_cols
    tile = min(512, columns)
    return pl.pallas_call(
        share_kernel,
        grid=(columns // tile,),
        in_specs=[
            pl.BlockSpec((text.shape[0], tile), lambda i: (0, i)),
            pl.BlockSpec((image.shape[0], tile), lambda i: (0, i)),
            pl.BlockSpec(back.shape, lambda i: (0, 0)),
            pl.BlockSpec(image_back.shape, lambda i: (0, 0)),
        ],
        out_specs=pl.BlockSpec((heads, tile, head_cols), lambda i: (0, i, 0)),
        out_shape=jax.ShapeDtypeStruct((heads, columns, head_cols), jnp.bfloat16),
        cost_estimate=pl.CostEstimate(
            flops=2 * (text.size + image.size) * back.shape[1],
            bytes_accessed=2 * (text.size + image.size + columns * back.shape[1]),
            transcendentals=0,
        ),
    )(text, image, back, image_back)


def project_kernel(text_ref, image_ref, weight_ref, out_ref):
    step = pl.program_id(0)
    last = pl.num_programs(0) - 1
    rows = jnp.where(step == last, image_ref[...], text_ref[...])
    part = jnp.dot(rows, weight_ref[...], preferred_element_type=jnp.float32).astype(out_ref.dtype)
    width = out_ref.shape[2]
    for head in range(out_ref.shape[0]):
        out_ref[head] = part[:, head * width : (head + 1) * width]


def projection_parts(text, image, weight, head_cols):
    heads = weight.shape[1] // head_cols
    tile, columns = image.shape
    text_tiles = text.shape[0] // tile
    return pl.pallas_call(
        project_kernel,
        grid=(text_tiles + 1,),
        in_specs=[
            pl.BlockSpec((tile, columns), lambda i: (jnp.minimum(i, text_tiles - 1), 0)),
            pl.BlockSpec((tile, columns), lambda i: (0, 0)),
            pl.BlockSpec(weight.shape, lambda i: (0, 0)),
        ],
        out_specs=pl.BlockSpec((heads, tile, head_cols), lambda i: (0, i, 0)),
        out_shape=jax.ShapeDtypeStruct((heads, text.shape[0] + tile, head_cols), jnp.bfloat16),
        cost_estimate=pl.CostEstimate(
            flops=2 * (text.size + image.size) * weight.shape[1],
            bytes_accessed=2 * (text.size + image.size + weight.size),
            transcendentals=0,
        ),
    )(text, image, weight)


def spread(piece, axis):
    count = lax.axis_size(axis)
    copies = jnp.broadcast_to(piece[None], (count,) + piece.shape)
    got = lax.all_to_all(copies, axis, split_axis=0, concat_axis=0, tiled=True)
    return got.reshape((count * piece.shape[0],) + piece.shape[1:])


def per_device(
    text_embeds, image_embeds, key_weight, key_bias, key_cot, image_owner, image_slot, seq_lengths
):
    row_count, columns = text_embeds.shape
    image_count = image_embeds.shape[0]
    units = ("group", "fsdp")
    core_count = lax.axis_size("group")
    fsdp_count = lax.axis_size("fsdp")
    tp_count = lax.axis_size("tp")
    unit_count = core_count * fsdp_count
    capacity = row_count // unit_count
    slot_count = unit_count * capacity
    head_cols = key_bias.shape[0]
    key_cols = head_cols * tp_count
    weight_block = key_weight.shape[0]
    halves = unit_count // tp_count
    tp_index = lax.axis_index("tp")

    position = jnp.arange(row_count, dtype=jnp.int32)
    seq_ids = position // LENGTH
    seq_marks = seq_ids[:, None] == jnp.arange(seq_lengths.shape[0], dtype=jnp.int32)[None, :]
    live_limit = jnp.sum(jnp.where(seq_marks, seq_lengths[None, :], 0), axis=1)
    live_mask = (position % LENGTH < live_limit).astype(jnp.float32)
    cosine, sine = angles(row_count)
    masked = key_cot.astype(jnp.float32) * live_mask[:, None]
    rotated_back = rotate(masked, cosine, sine, -1.0).astype(jnp.bfloat16)
    is_image = image_slot >= 0
    text_back = jnp.where(is_image[:, None], jnp.zeros_like(rotated_back), rotated_back)

    slot_ids = jnp.arange(slot_count, dtype=jnp.int32)
    place = (image_slot[:, None] == slot_ids[None, :]).astype(jnp.bfloat16)
    returning = lax.dot_general(
        place, rotated_back, (((0,), (0,)), ((), ())), preferred_element_type=jnp.float32
    ).astype(jnp.bfloat16)
    returned = lax.all_to_all(
        returning.reshape(unit_count, capacity, key_cols), units, split_axis=0, concat_axis=0,
        tiled=True,
    ).reshape(slot_count, key_cols)
    slots_out = send_slots(image_owner, unit_count, capacity)
    pick = (slots_out[:, None] == slot_ids[None, :]).astype(jnp.bfloat16)
    image_back = jnp.dot(pick, returned, preferred_element_type=jnp.float32).astype(jnp.bfloat16)

    piece_rows = weight_block // tp_count
    own_piece = lax.dynamic_slice_in_dim(key_weight, tp_index * piece_rows, piece_rows, 0)
    moves = []
    for unit in range(unit_count):
        for part in range(tp_count):
            target = (unit % halves) * tp_count + part
            moves.append((unit * tp_count + part, target * tp_count + unit // halves))
    own_piece = lax.ppermute(own_piece, units + ("tp",), moves)
    weight_rows = spread(spread(own_piece, "fsdp"), "group")

    shares = weight_shares(text_embeds, image_embeds, text_back, image_back, head_cols)
    shares = shares.reshape(core_count, fsdp_count, weight_block, head_cols)
    shares = lax.all_to_all(shares, "group", split_axis=0, concat_axis=0, tiled=True)
    shares = jnp.sum(shares.astype(jnp.float32), axis=0).astype(jnp.bfloat16)
    shares = lax.all_to_all(shares, "fsdp", split_axis=0, concat_axis=0, tiled=True)
    weight_grad = jnp.sum(shares.astype(jnp.float32), axis=0) / row_count
    returns = []
    for unit in range(unit_count):
        for part in range(tp_count):
            holder = (unit % halves) + part * halves
            returns.append((holder * tp_count + unit // halves, unit * tp_count + part))
    weight_grad = lax.ppermute(weight_grad, units + ("tp",), returns)

    both = projection_parts(text_embeds, image_embeds, weight_rows, head_cols)
    both = lax.all_to_all(both, "tp", split_axis=0, concat_axis=0, tiled=True)
    both = jnp.sum(both.astype(jnp.float32), axis=0)
    image_proj = both[row_count:].astype(jnp.bfloat16)
    outgoing = lax.dot_general(
        pick, image_proj, (((0,), (0,)), ((), ())), preferred_element_type=jnp.float32
    ).astype(jnp.bfloat16)
    received = lax.all_to_all(
        outgoing.reshape(unit_count, capacity, head_cols), units, split_axis=0, concat_axis=0,
        tiled=True,
    ).reshape(slot_count, head_cols)
    placed = jnp.dot(place, received, preferred_element_type=jnp.float32)
    projected = jnp.where(is_image[:, None], placed, both[:row_count]) + key_bias
    key_rows = (rotate(projected, cosine, sine, 1.0) * live_mask[:, None]).astype(jnp.bfloat16)

    contract = (((1,), (1,)), ((), ()))
    text_grad = lax.dot_general(
        text_back, weight_rows, contract, preferred_element_type=jnp.float32
    ).astype(jnp.bfloat16)
    image_grad = lax.dot_general(
        image_back, weight_rows, contract, preferred_element_type=jnp.float32
    ).astype(jnp.bfloat16)
    return (key_rows, text_grad, image_grad, weight_grad)


def solution(mesh):
    in_specs = (
        P(("group", "fsdp"), "tp"),
        P(("group", "fsdp"), "tp"),
        P(("group", "fsdp"), None),
        P("tp"),
        P(("group", "fsdp"), None),
        P(("group", "fsdp")),
        P(("group", "fsdp")),
        P(("group", "fsdp")),
    )
    out_specs = (
        P(("group", "fsdp"), "tp"),
        P(("group", "fsdp"), "tp"),
        P(("group", "fsdp"), "tp"),
        P(("group", "fsdp"), "tp"),
    )
    return jax.shard_map(
        per_device, mesh=mesh, in_specs=in_specs, out_specs=out_specs, check_vma=False
    )
```

```python
import jax
import jax.numpy as jnp
from jax import lax
from jax.experimental import pallas as pl
from jax.experimental.pallas import tpu as pltpu
from jax.sharding import PartitionSpec as P

HEAD_DIM = 128
LENGTH = 256


ROPE_BASE = 1000000.0


def angles(row_total):
    position = (jnp.arange(row_total, dtype=jnp.int32) % LENGTH).astype(jnp.float32)
    frequency = ROPE_BASE ** (-(jnp.arange(HEAD_DIM // 2, dtype=jnp.float32) * 2.0) / HEAD_DIM)
    angle_table = position[:, None] * frequency[None, :]
    return (jnp.cos(angle_table), jnp.sin(angle_table))


def rotate(values, cosine, sine, direction):
    row_total = values.shape[0]
    by_head = values.reshape(row_total, -1, HEAD_DIM)
    half_dim = HEAD_DIM // 2
    front_half = by_head[..., :half_dim]
    second = by_head[..., half_dim:]
    cos_part = cosine[:, None, :]
    sin_part = direction * sine[:, None, :]
    rotated = jnp.concatenate(
        [front_half * cos_part - second * sin_part, second * cos_part + front_half * sin_part],
        axis=-1,
    )
    return rotated.reshape(row_total, -1)


def send_slots(owners, unit_count, capacity):
    onehot_marks = (owners[:, None] == jnp.arange(unit_count, dtype=jnp.int32)[None, :]).astype(
        jnp.int32
    )
    before = jnp.cumsum(onehot_marks, axis=0) - onehot_marks
    owner_rank = jnp.sum(before * onehot_marks, axis=1)
    return owners * capacity + owner_rank


def share_kernel(text_ref, image_ref, back_ref, image_back_ref, out_ref):
    contract = (((0,), (0,)), ((), ()))
    part = lax.dot_general(
        text_ref[...], back_ref[...], contract, preferred_element_type=jnp.float32
    ) + lax.dot_general(
        image_ref[...], image_back_ref[...], contract, preferred_element_type=jnp.float32
    )
    part = part.astype(out_ref.dtype)
    width = out_ref.shape[2]
    for head in range(out_ref.shape[0]):
        out_ref[head] = part[:, head * width : (head + 1) * width]


def weight_shares(text, image, back, image_back, head_cols):
    columns = text.shape[1]
    heads = back.shape[1] // head_cols
    tile = min(512, columns)
    return pl.pallas_call(
        share_kernel,
        grid=(columns // tile,),
        in_specs=[
            pl.BlockSpec((text.shape[0], tile), lambda i: (0, i)),
            pl.BlockSpec((image.shape[0], tile), lambda i: (0, i)),
            pl.BlockSpec(back.shape, lambda i: (0, 0)),
            pl.BlockSpec(image_back.shape, lambda i: (0, 0)),
        ],
        out_specs=pl.BlockSpec((heads, tile, head_cols), lambda i: (0, i, 0)),
        out_shape=jax.ShapeDtypeStruct((heads, columns, head_cols), jnp.bfloat16),
        cost_estimate=pl.CostEstimate(
            flops=2 * (text.size + image.size) * back.shape[1],
            bytes_accessed=2 * (text.size + image.size + columns * back.shape[1]),
            transcendentals=0,
        ),
    )(text, image, back, image_back)


def project_kernel(text_ref, image_ref, weight_ref, out_ref):
    step = pl.program_id(0)
    last = pl.num_programs(0) - 1
    rows = jnp.where(step == last, image_ref[...], text_ref[...])
    part = jnp.dot(rows, weight_ref[...], preferred_element_type=jnp.float32).astype(out_ref.dtype)
    width = out_ref.shape[2]
    for head in range(out_ref.shape[0]):
        out_ref[head] = part[:, head * width : (head + 1) * width]


def projection_parts(text, image, weight, head_cols):
    heads = weight.shape[1] // head_cols
    tile, columns = image.shape
    text_tiles = text.shape[0] // tile
    return pl.pallas_call(
        project_kernel,
        grid=(text_tiles + 1,),
        in_specs=[
            pl.BlockSpec((tile, columns), lambda i: (jnp.minimum(i, text_tiles - 1), 0)),
            pl.BlockSpec((tile, columns), lambda i: (0, 0)),
            pl.BlockSpec(weight.shape, lambda i: (0, 0)),
        ],
        out_specs=pl.BlockSpec((heads, tile, head_cols), lambda i: (0, i, 0)),
        out_shape=jax.ShapeDtypeStruct((heads, text.shape[0] + tile, head_cols), jnp.bfloat16),
        cost_estimate=pl.CostEstimate(
            flops=2 * (text.size + image.size) * weight.shape[1],
            bytes_accessed=2 * (text.size + image.size + weight.size),
            transcendentals=0,
        ),
    )(text, image, weight)


def spread(piece, axis):
    count = lax.axis_size(axis)
    copies = jnp.broadcast_to(piece[None], (count,) + piece.shape)
    got = lax.all_to_all(copies, axis, split_axis=0, concat_axis=0, tiled=True)
    return got.reshape((count * piece.shape[0],) + piece.shape[1:])


def shifted(values, axis, step):
    count = lax.axis_size(axis)
    return lax.ppermute(values, axis, [(i, (i + step) % count) for i in range(count)])


def exchange_sum(blocks, axis):
    count = lax.axis_size(axis)
    me = lax.axis_index(axis)
    total = lax.dynamic_index_in_dim(blocks, me, 0, keepdims=False).astype(jnp.float32)
    for step in range(1, count):
        block = lax.dynamic_index_in_dim(blocks, (me + step) % count, 0, keepdims=False)
        total = total + shifted(block, axis, step).astype(jnp.float32)
    return total


def share_rows(piece, axis):
    count = lax.axis_size(axis)
    me = lax.axis_index(axis)
    rows = piece.shape[0]
    full = jnp.zeros((count * rows,) + piece.shape[1:], piece.dtype)
    full = lax.dynamic_update_slice_in_dim(full, piece, me * rows, 0)
    for step in range(1, count):
        source = (me + count - step) % count
        full = lax.dynamic_update_slice_in_dim(full, shifted(piece, axis, step), source * rows, 0)
    return full


def per_device(
    text_embeds, image_embeds, key_weight, key_bias, key_cot, image_owner, image_slot, seq_lengths
):
    row_count, columns = text_embeds.shape
    image_count = image_embeds.shape[0]
    units = ("group", "fsdp")
    core_count = lax.axis_size("group")
    fsdp_count = lax.axis_size("fsdp")
    tp_count = lax.axis_size("tp")
    unit_count = core_count * fsdp_count
    capacity = row_count // unit_count
    slot_count = unit_count * capacity
    head_cols = key_bias.shape[0]
    key_cols = head_cols * tp_count
    weight_block = key_weight.shape[0]
    halves = unit_count // tp_count
    tp_index = lax.axis_index("tp")

    position = jnp.arange(row_count, dtype=jnp.int32)
    seq_ids = position // LENGTH
    seq_marks = seq_ids[:, None] == jnp.arange(seq_lengths.shape[0], dtype=jnp.int32)[None, :]
    live_limit = jnp.sum(jnp.where(seq_marks, seq_lengths[None, :], 0), axis=1)
    live_mask = (position % LENGTH < live_limit).astype(jnp.float32)
    cosine, sine = angles(row_count)
    masked = key_cot.astype(jnp.float32) * live_mask[:, None]
    rotated_back = rotate(masked, cosine, sine, -1.0).astype(jnp.bfloat16)
    is_image = image_slot >= 0
    text_back = jnp.where(is_image[:, None], jnp.zeros_like(rotated_back), rotated_back)

    slot_ids = jnp.arange(slot_count, dtype=jnp.int32)
    place = (image_slot[:, None] == slot_ids[None, :]).astype(jnp.bfloat16)
    returning = lax.dot_general(
        place, rotated_back, (((0,), (0,)), ((), ())), preferred_element_type=jnp.float32
    ).astype(jnp.bfloat16)
    returned = lax.all_to_all(
        returning.reshape(unit_count, capacity, key_cols), units, split_axis=0, concat_axis=0,
        tiled=True,
    ).reshape(slot_count, key_cols)
    slots_out = send_slots(image_owner, unit_count, capacity)
    pick = (slots_out[:, None] == slot_ids[None, :]).astype(jnp.bfloat16)
    image_back = jnp.dot(pick, returned, preferred_element_type=jnp.float32).astype(jnp.bfloat16)

    piece_rows = weight_block // tp_count
    own_piece = lax.dynamic_slice_in_dim(key_weight, tp_index * piece_rows, piece_rows, 0)
    moves = []
    for unit in range(unit_count):
        for part in range(tp_count):
            target = (unit % halves) * tp_count + part
            moves.append((unit * tp_count + part, target * tp_count + unit // halves))
    own_piece = lax.ppermute(own_piece, units + ("tp",), moves)
    chip_rows = spread(own_piece, "fsdp")

    shares = weight_shares(text_embeds, image_embeds, text_back, image_back, head_cols)
    shares = shares.reshape(core_count, fsdp_count, weight_block, head_cols)
    shares = exchange_sum(shares, "group").astype(jnp.bfloat16)
    shares, chip_rows = lax.optimization_barrier((shares, chip_rows))
    shares = lax.all_to_all(shares, "fsdp", split_axis=0, concat_axis=0, tiled=True)
    weight_grad = jnp.sum(shares.astype(jnp.float32), axis=0) / row_count
    returns = []
    for unit in range(unit_count):
        for part in range(tp_count):
            holder = (unit % halves) + part * halves
            returns.append((holder * tp_count + unit // halves, unit * tp_count + part))
    weight_grad = lax.ppermute(weight_grad, units + ("tp",), returns)

    weight_rows = share_rows(chip_rows, "group")
    both = projection_parts(text_embeds, image_embeds, weight_rows, head_cols)
    both = exchange_sum(both, "tp")
    image_proj = both[row_count:].astype(jnp.bfloat16)
    outgoing = lax.dot_general(
        pick, image_proj, (((0,), (0,)), ((), ())), preferred_element_type=jnp.float32
    ).astype(jnp.bfloat16)
    received = lax.all_to_all(
        outgoing.reshape(unit_count, capacity, head_cols), units, split_axis=0, concat_axis=0,
        tiled=True,
    ).reshape(slot_count, head_cols)
    placed = jnp.dot(place, received, preferred_element_type=jnp.float32)
    projected = jnp.where(is_image[:, None], placed, both[:row_count]) + key_bias
    key_rows = (rotate(projected, cosine, sine, 1.0) * live_mask[:, None]).astype(jnp.bfloat16)

    contract = (((1,), (1,)), ((), ()))
    text_grad = lax.dot_general(
        text_back, weight_rows, contract, preferred_element_type=jnp.float32
    ).astype(jnp.bfloat16)
    image_grad = lax.dot_general(
        image_back, weight_rows, contract, preferred_element_type=jnp.float32
    ).astype(jnp.bfloat16)
    return (key_rows, text_grad, image_grad, weight_grad)


def solution(mesh):
    in_specs = (
        P(("group", "fsdp"), "tp"),
        P(("group", "fsdp"), "tp"),
        P(("group", "fsdp"), None),
        P("tp"),
        P(("group", "fsdp"), None),
        P(("group", "fsdp")),
        P(("group", "fsdp")),
        P(("group", "fsdp")),
    )
    out_specs = (
        P(("group", "fsdp"), "tp"),
        P(("group", "fsdp"), "tp"),
        P(("group", "fsdp"), "tp"),
        P(("group", "fsdp"), "tp"),
    )
    return jax.shard_map(
        per_device, mesh=mesh, in_specs=in_specs, out_specs=out_specs, check_vma=False
    )
```
